32 devices in a mesh: ka: 8 (over z, core), band: 4 (over y, x).
Axes of the slice: x: 2, y: 2, z: 4, core: 2. Of those that a mesh axis runs over, the one named last changes fastest.
Arguments:
- occ_rows: bfloat16 [8, 2048, 128], P('ka', 'band'), may hold values from -0.5 to 0.5
- vir_rows: bfloat16 [8, 2048, 896], P('ka', 'band'), may hold values from -0.1875 to 0.1875
- trial_vectors: float32 [8, 2, 128, 896], P('ka', None, None, 'band'), may hold values from -6 to 6
- occ_energy: float32 [8, 128], P('ka'), may hold values from -1.2 to -0.3
- vir_energy: float32 [8, 896], P('ka', 'band'), may hold values from 0.1 to 1.5
- coulomb: bfloat16 [2048, 2048], P('band'), may hold values from -0.09375 to 0.09375
- exch_kernel: bfloat16 [8, 2048, 2048], P(None, 'band'), as said below
- minus_table: int32 [8, 8], replicated, may hold values from 0 to 7, as said below
Outputs:
- sigma_vectors: float32 [8, 2, 128, 896], P('ka', None, None, 'band')
The draws below stay inside these ranges and needn't reach their ends.
Inputs may be any that keep to these rules, and one draw needn't show every extreme that they name: minus_table[k, q] is the k-point k - q on a group of 8 k-points: every row and every column holds each index once, and one q gives minus_table[k, q] == k for every k. Each exch_kernel[q] is symmetric.
All inputs are finite; a program needn't handle non-finite values.
Results may differ from the reference program's by a relative error of at most 0.0051.
Values may be sent and summed in bfloat16 or wider, within the bound.
A program may use at most 128 MiB of HBM per device.

```python
import jax
import jax.numpy as jnp
from jax import lax

NOCC = 128
NVIR = 896
NAUX = 2048
NVEC = 2
NK = 8


def draw_minus_table(key, part):
    labels = jax.random.permutation(jax.random.fold_in(key, 11), NK).astype(jnp.int32)
    difference = (labels[:, None] - labels[None, :]) % NK
    inverse = jnp.argsort(labels).astype(jnp.int32)
    return inverse[difference].astype(jnp.int32)


def draw_exch_kernel(key, part):
    spread = jnp.sqrt(jnp.float32(NOCC) / jnp.float32(NK * NAUX))
    base = jax.random.normal(jax.random.fold_in(key, 3), (NK, NAUX, NAUX), jnp.float32)
    symmetric = (base + jnp.transpose(base, (0, 2, 1))) * 0.7071
    return (symmetric * spread).astype(jnp.bfloat16)


def levels(stream_key, shape, split, smallest, high):
    factor_of = 1.0
    for position, blocks in split:
        draws = jax.random.uniform(jax.random.fold_in(jax.random.fold_in(stream_key, 6), position), (blocks,), jnp.float32, smallest / len(split), high / len(split))
        factor_of = factor_of * jnp.repeat(jnp.exp(draws), shape[position] // blocks).reshape((-1,) + (1,) * (len(shape) - 1 - position))
    return factor_of


def normal_values(key, shape, scale, reach, shards=(), held_as=jnp.bfloat16):
    result = scale * jax.random.normal(key, shape, jnp.float32)
    if shards:
        result = result * levels(key, shape, shards, -0.22, 0.18)
    return jnp.clip(result, -reach, reach).astype(held_as)


def setup_inputs(seed: int = 0) -> dict:
    key_list = jax.random.split(jax.random.key(seed), 9)
    occ_rows = normal_values(key_list[0], (NK, NAUX, NOCC), NOCC ** -0.5, 0.5, ((0, 8), (1, 4)))
    vir_rows = normal_values(key_list[1], (NK, NAUX, NVIR), NVIR ** -0.5, 0.1875, ((0, 8), (1, 4)))
    trial_vectors = normal_values(key_list[2], (NK, NVEC, NOCC, NVIR), 1.0, 6.0, ((0, 8), (3, 4)), jnp.float32)
    occ_energy = jnp.clip(-1.2 + 0.90000004 * jax.random.uniform(key_list[3], (NK, NOCC), jnp.float32) ** levels(key_list[3], (NK, NOCC), ((0, 8),), -0.2, 0.2), -1.2, -0.3)
    vir_energy = jnp.clip(0.1 + 1.4 * jax.random.uniform(key_list[4], (NK, NVIR), jnp.float32) ** levels(key_list[4], (NK, NVIR), ((0, 8), (1, 4)), -0.2, 0.2), 0.1, 1.5)
    coulomb = normal_values(key_list[5], (NAUX, NAUX), (NK * NAUX // 4) ** -0.5, 0.09375, ((0, 4),))
    exch_kernel = draw_exch_kernel(jax.random.fold_in(key_list[8], 71), 0)
    minus_table = draw_minus_table(jax.random.fold_in(key_list[8], 71), 0)
    return dict(occ_rows=occ_rows, vir_rows=vir_rows, trial_vectors=trial_vectors, occ_energy=occ_energy, vir_energy=vir_energy, coulomb=coulomb, exch_kernel=exch_kernel, minus_table=minus_table)


def reference(occ_rows, vir_rows, trial_vectors, occ_energy, vir_energy, coulomb, exch_kernel, minus_table):
    highest = lax.Precision.HIGHEST
    trial_half = trial_vectors.astype(jnp.bfloat16)

    def build_pairs(kpoint):
        occ_here = occ_rows[kpoint].astype(jnp.float32)
        vir_here = vir_rows[kpoint].astype(jnp.float32)
        mixed_rows = jnp.einsum("ri,via->vra", occ_here, trial_half[kpoint].astype(jnp.float32), precision=highest)
        mixed_rows = mixed_rows.astype(jnp.bfloat16)
        pair_block = jnp.einsum("vra,na->vrn", mixed_rows.astype(jnp.float32), vir_here, precision=highest)
        density_here = jnp.sum(mixed_rows.astype(jnp.float32) * vir_here[None], axis=2)
        return pair_block.astype(jnp.bfloat16), density_here

    pair_blocks, densities = lax.map(build_pairs, jnp.arange(NK, dtype=jnp.int32))
    density_half = jnp.sum(densities, axis=0).astype(jnp.bfloat16)
    potential = jnp.einsum("vn,rn->vr", density_half.astype(jnp.float32), coulomb.astype(jnp.float32), precision=highest)

    def build_sigma(kpoint):
        def add_transfer(running, momentum):
            source = minus_table[kpoint, momentum]
            weighted = pair_blocks[source].astype(jnp.float32) * exch_kernel[momentum].astype(jnp.float32)[None]
            return running + weighted, None

        screened, unused = lax.scan(add_transfer, jnp.zeros((NVEC, NAUX, NAUX), jnp.float32), jnp.arange(NK, dtype=jnp.int32))
        screened = screened.astype(jnp.bfloat16)
        vir_here = vir_rows[kpoint].astype(jnp.float32)
        product = jnp.einsum("vrn,na->vra", screened.astype(jnp.float32), vir_here, precision=highest)
        weights = (2.0 * potential[:, :, None] * vir_here[None] - product).astype(jnp.bfloat16)
        coupled = jnp.einsum("ri,vra->via", occ_rows[kpoint].astype(jnp.float32), weights.astype(jnp.float32), precision=highest)
        energy_gaps = vir_energy[kpoint][None, :] - occ_energy[kpoint][:, None]
        return energy_gaps[None] * trial_vectors[kpoint] + coupled

    return lax.map(build_sigma, jnp.arange(NK, dtype=jnp.int32))
```

```python
import functools

import jax
import jax.numpy as jnp
from jax import lax
from jax.experimental import pallas as pl
from jax.experimental.pallas import tpu as pltpu
from jax.sharding import PartitionSpec as P

F32 = jnp.float32
BF16 = jnp.bfloat16
CHUNK = 16


def dot_nt(left, right, **options):
    return lax.dot_general(
        left, right, (((1,), (1,)), ((), ())), preferred_element_type=F32, **options
    )


def kernel(
    kpoints,
    bands,
    vectors,
    occ,
    vir,
    trial,
    coulomb,
    exch,
    table,
    out,
    occ_full,
    occ_tile,
    trial_all,
    half_own,
    half_all,
    dens_all,
    dens_band,
    coulomb_here,
    exch_tile,
    pairs,
    screened,
    sums_send,
    sums_recv,
    sigma_send,
    sigma_recv,
    local_sem,
    occ_band_sem,
    trial_sem,
    occ_point_sem,
    occ_pass_sem,
    half_sem,
    dens_sem,
    dens_band_sem,
    sums_sem,
    sigma_sem,
):
    me = lax.axis_index("ka")
    band = lax.axis_index("band")
    groups = kpoints // 2
    group = lax.div(me, 2)
    core = lax.rem(me, 2)
    sibling = me + 1 - 2 * core
    rows, occupied = occ.shape
    auxiliary = occ_full.shape[0]
    half = rows // 2
    width = auxiliary // groups

    def remote(source, target, sems, slot, device):
        return pltpu.make_async_remote_copy(
            src_ref=source,
            dst_ref=target,
            send_sem=sems.at[0, slot],
            recv_sem=sems.at[1, slot],
            device_id=device,
            device_id_type=pl.DeviceIdType.MESH,
        )

    exch_copy = pltpu.make_async_copy(
        exch.at[
            :,
            pl.ds(pl.multiple_of(core * half, half), half),
            pl.ds(pl.multiple_of(group * width, width), width),
        ],
        exch_tile,
        local_sem.at[0],
    )
    exch_copy.start()
    coulomb_copy = pltpu.make_async_copy(coulomb, coulomb_here, local_sem.at[1])
    coulomb_copy.start()

    barrier = pltpu.get_barrier_semaphore()
    for step in range(1, bands):
        pl.semaphore_signal(
            barrier,
            inc=1,
            device_id=(me, lax.rem(band + step, bands)),
            device_id_type=pl.DeviceIdType.MESH,
        )
    for step in range(1, kpoints):
        pl.semaphore_signal(
            barrier,
            inc=1,
            device_id=(lax.rem(me + step, kpoints), band),
            device_id_type=pl.DeviceIdType.MESH,
        )
    pl.semaphore_wait(barrier, bands + kpoints - 2)

    own_rows = pl.ds(pl.multiple_of(band * rows, rows), rows)
    trial_copies = []
    for step in range(1, bands):
        copy = remote(
            trial, trial_all.at[band], trial_sem, step, (me, lax.rem(band + step, bands))
        )
        copy.start()
        trial_copies.append(copy)
    occ_copies = []
    for step in range(1, bands):
        copy = remote(
            occ, occ_full.at[own_rows], occ_band_sem, step, (me, lax.rem(band + step, bands))
        )
        copy.start()
        occ_copies.append(copy)
    occ_full[own_rows, :] = occ[...]
    trial_all[band] = trial[...]

    for copy in trial_copies:
        copy.wait_recv()
    product = dot_nt(vir[0], trial_all[0])
    for part in range(1, bands):
        product += dot_nt(vir[part], trial_all[part])
    half_own[...] = product.astype(BF16)
    half_all[me] = half_own[pl.ds(pl.multiple_of(core * half, half), half), :]
    half_copies = []
    for step in range(1, kpoints):
        peer = lax.rem(me + step, kpoints)
        peer_core = lax.rem(peer, 2)
        copy = remote(
            half_own.at[pl.ds(pl.multiple_of(peer_core * half, half), half)],
            half_all.at[me],
            half_sem,
            step,
            (peer, band),
        )
        copy.start()
        half_copies.append(copy)

    for copy in occ_copies:
        copy.wait_recv()
    point_copies = []
    for step in range(1, groups):
        peer_group = lax.rem(group + step, groups)
        copy = remote(
            occ_full.at[pl.ds(pl.multiple_of(peer_group * width, width), width)],
            occ_tile.at[me],
            occ_point_sem,
            step,
            (peer_group * 2 + core, band),
        )
        copy.start()
        point_copies.append(copy)
    occ_tile[me] = occ_full[pl.ds(pl.multiple_of(group * width, width), width), :]
    pass_copies = [
        remote(
            occ_full.at[pl.ds(pl.multiple_of(group * width, width), width)],
            occ_tile.at[me],
            occ_pass_sem,
            0,
            (sibling, band),
        )
    ]
    pass_copies[0].start()

    ones = jnp.ones((8, occupied), F32)
    occ_wide = occ[...].astype(F32)
    line = lax.broadcasted_iota(jnp.int32, (8, rows), 0)
    density = jnp.zeros((8, rows), F32)
    for v in range(vectors):
        here = half_own[:, v * occupied : (v + 1) * occupied].astype(F32)
        summed = dot_nt(ones, occ_wide * here, precision=lax.Precision.HIGHEST)
        density = jnp.where(line == v, summed, density)
    dens_all[me] = density
    dens_copies = []
    for step in range(1, kpoints):
        copy = remote(
            dens_all.at[me],
            dens_all.at[me],
            dens_sem,
            step,
            (lax.rem(me + step, kpoints), band),
        )
        copy.start()
        dens_copies.append(copy)

    for step in range(1, groups):
        point_copies[step - 1].wait_recv()
        source = lax.rem(group - step + groups, groups) * 2 + core
        copy = remote(
            occ_tile.at[source], occ_tile.at[source], occ_pass_sem, step, (sibling, band)
        )
        copy.start()
        pass_copies.append(copy)

    for copy in dens_copies:
        copy.wait_recv()
    density = dens_all[0]
    for k in range(1, kpoints):
        density += dens_all[k]
    dens_band[band] = jnp.concatenate([density, jnp.zeros_like(density)], axis=0).astype(BF16)
    dens_band_copies = []
    for step in range(1, bands):
        copy = remote(
            dens_band.at[band],
            dens_band.at[band],
            dens_band_sem,
            step,
            (me, lax.rem(band + step, bands)),
        )
        copy.start()
        dens_band_copies.append(copy)

    for copy in pass_copies:
        copy.wait_recv()
    exch_copy.wait()

    for step in range(kpoints):
        if step:
            half_copies[step - 1].wait_recv()
        source = lax.rem(me - step + kpoints, kpoints)
        for v in range(vectors):
            pairs[source * vectors + v] = dot_nt(
                half_all[source, :, v * occupied : (v + 1) * occupied], occ_tile[source]
            )

    def screen(target):
        sources = [table[target, q] * vectors for q in range(kpoints)]

        def add_rows(chunk, carry):
            here = pl.ds(pl.multiple_of(chunk * CHUNK, CHUNK), CHUNK)
            totals = [jnp.zeros((CHUNK, width), F32) for _ in range(vectors)]
            for q in range(kpoints):
                factor = exch_tile[q, here, :].astype(F32)
                for v in range(vectors):
                    totals[v] += pairs[sources[q] + v, here, :] * factor
            for v in range(vectors):
                screened[v, here, :] = totals[v].astype(BF16)
            return carry

        lax.fori_loop(0, half // CHUNK, add_rows, 0)
        return jnp.concatenate(
            [
                jnp.dot(screened[v], occ_tile[target], preferred_element_type=F32)
                for v in range(vectors)
            ],
            axis=1,
        ).astype(BF16)

    def sums_copy(step):
        target = lax.rem(me + 1 + step, kpoints)
        return remote(
            sums_send.at[target], sums_recv.at[me], sums_sem, step, (target, band)
        )

    def make_sums(step, carry):
        target = lax.rem(me + 1 + step, kpoints)
        sums_send[target] = screen(target)
        sums_copy(step).start()
        return carry

    lax.fori_loop(0, kpoints - 1, make_sums, 0)
    sums_recv[me] = screen(me)

    for copy in dens_band_copies:
        copy.wait_recv()
    coulomb_copy.wait()
    potential = dot_nt(coulomb_here[:, :rows], dens_band[0])
    for part in range(1, bands):
        potential += dot_nt(coulomb_here[:, part * rows : (part + 1) * rows], dens_band[part])
    for step in range(kpoints - 1):
        sums_copy(step).wait_recv()
    pieces = []
    for side in range(2):
        total = sums_recv[side].astype(F32)
        for g in range(1, groups):
            total += sums_recv[2 * g + side].astype(F32)
        lines = slice(side * half, (side + 1) * half)
        direct = [
            2.0 * potential[lines, v : v + 1] * occ_wide[lines] for v in range(vectors)
        ]
        pieces.append(jnp.concatenate(direct, axis=1) - total)
    coupling = jnp.concatenate(pieces, axis=0).T.astype(BF16)

    sigma_copies = []
    for step in range(1, bands):
        peer = lax.rem(band + step, bands)
        sigma_send[step] = jnp.dot(coupling, vir[peer], preferred_element_type=F32).astype(BF16)
        copy = remote(sigma_send.at[step], sigma_recv.at[step], sigma_sem, step, (me, peer))
        copy.start()
        sigma_copies.append(copy)
    result = jnp.dot(coupling, vir[band], preferred_element_type=F32)
    for step in range(1, bands):
        sigma_copies[step - 1].wait_recv()
        result += sigma_recv[step].astype(F32)
    out[...] = result

    for copy in (
        trial_copies
        + occ_copies
        + half_copies
        + point_copies
        + pass_copies
        + dens_copies
        + dens_band_copies
        + sigma_copies
        + [sums_copy(step) for step in range(kpoints - 1)]
    ):
        copy.wait_send()


def coupled_part(kpoints, bands, occ, vir, trial, coulomb, exch, table, vectors):
    rows, occupied = occ.shape
    merged, columns = trial.shape
    auxiliary = coulomb.shape[1]
    half = rows // 2
    width = auxiliary * 2 // kpoints
    vmem = pl.BlockSpec(memory_space=pltpu.VMEM)
    hbm = pl.BlockSpec(memory_space=pl.ANY)
    smem = pl.BlockSpec(memory_space=pltpu.SMEM)
    both = pltpu.SemaphoreType.DMA
    return pl.pallas_call(
        functools.partial(kernel, kpoints, bands, vectors),
        out_shape=jax.ShapeDtypeStruct((merged, columns), F32),
        in_specs=[vmem, vmem, vmem, hbm, hbm, smem],
        out_specs=vmem,
        scratch_shapes=[
            pltpu.VMEM((auxiliary, occupied), BF16),
            pltpu.VMEM((kpoints, width, occupied), BF16),
            pltpu.VMEM((bands, merged, columns), BF16),
            pltpu.VMEM((rows, merged), BF16),
            pltpu.VMEM((kpoints, half, merged), BF16),
            pltpu.VMEM((kpoints, 8, rows), F32),
            pltpu.VMEM((bands, 16, rows), BF16),
            pltpu.VMEM((rows, auxiliary), BF16),
            pltpu.VMEM((kpoints, half, width), BF16),
            pltpu.VMEM((kpoints * vectors, half, width), F32),
            pltpu.VMEM((vectors, half, width), BF16),
            pltpu.VMEM((kpoints, half, merged), BF16),
            pltpu.VMEM((kpoints, half, merged), BF16),
            pltpu.VMEM((bands, merged, columns), BF16),
            pltpu.VMEM((bands, merged, columns), BF16),
            both((2,)),
            both((2, bands)),
            both((2, bands)),
            both((2, kpoints)),
            both((2, kpoints)),
            both((2, kpoints)),
            both((2, kpoints)),
            both((2, bands)),
            both((2, kpoints)),
            both((2, bands)),
        ],
        compiler_params=pltpu.CompilerParams(
            collective_id=0, has_side_effects=True, vmem_limit_bytes=60 * 2**20
        ),
        name="coupled",
    )(occ, vir, trial, coulomb, exch, table)


def per_device(
    occ_rows, vir_rows, trial_vectors, occ_energy, vir_energy, coulomb, exch_kernel, minus_table
):
    kpoints = lax.axis_size("ka")
    bands = lax.axis_size("band")
    _, vectors, occupied, columns = trial_vectors.shape
    rows = occ_rows.shape[1]
    trial_half = trial_vectors[0].astype(BF16).reshape(vectors * occupied, columns)
    vir_parts = vir_rows[0].reshape(rows, bands, columns).transpose(1, 0, 2)
    coupled = coupled_part(
        kpoints,
        bands,
        occ_rows[0],
        vir_parts,
        trial_half,
        coulomb,
        exch_kernel,
        minus_table,
        vectors,
    ).reshape(vectors, occupied, columns)
    energy_gaps = vir_energy[0][None, :] - occ_energy[0][:, None]
    return (energy_gaps[None] * trial_vectors[0] + coupled)[None]


def solution(mesh):
    in_specs = (
        P("ka", "band", None),
        P("ka", "band", None),
        P("ka", None, None, "band"),
        P("ka", None),
        P("ka", "band"),
        P("band", None),
        P(None, "band", None),
        P(),
    )
    out_specs = P("ka", None, None, "band")
    return jax.shard_map(
        per_device, mesh=mesh, in_specs=in_specs, out_specs=out_specs, check_vma=False
    )
```

```python
import functools

import jax
import jax.numpy as jnp
from jax import lax
from jax.experimental import pallas as pl
from jax.experimental.pallas import tpu as pltpu
from jax.sharding import PartitionSpec as P

F32 = jnp.float32
BF16 = jnp.bfloat16
CHUNK = 16


def dot_nt(left, right, **options):
    return lax.dot_general(
        left, right, (((1,), (1,)), ((), ())), preferred_element_type=F32, **options
    )


def kernel(
    kpoints,
    bands,
    vectors,
    occ,
    vir,
    trial,
    coulomb,
    exch,
    table,
    out,
    occ_full,
    occ_tile,
    trial_full,
    vir_turned,
    half_own,
    half_all,
    dens_all,
    dens_band,
    coulomb_here,
    exch_tile,
    pairs,
    screened,
    sums_send,
    sums_part,
    sums_recv,
    sigma_send,
    sigma_recv,
    local_sem,
    occ_band_sem,
    trial_sem,
    occ_point_sem,
    occ_pass_sem,
    half_sem,
    dens_sem,
    dens_band_sem,
    part_sem,
    sums_sem,
    sigma_sem,
):
    me = lax.axis_index("ka")
    band = lax.axis_index("band")
    groups = kpoints // 2
    group = lax.div(me, 2)
    core = lax.rem(me, 2)
    sibling = me + 1 - 2 * core
    rows, occupied = occ.shape
    auxiliary = occ_full.shape[0]
    half = rows // 2
    width = auxiliary // groups
    columns = trial.shape[1]
    own_columns = pl.ds(pl.multiple_of(band * columns, columns), columns)

    def remote(source, target, sems, slot, device, send_slot=None):
        return pltpu.make_async_remote_copy(
            src_ref=source,
            dst_ref=target,
            send_sem=sems.at[0, slot if send_slot is None else send_slot],
            recv_sem=sems.at[1, slot],
            device_id=device,
            device_id_type=pl.DeviceIdType.MESH,
        )

    exch_copy = pltpu.make_async_copy(
        exch.at[
            :,
            pl.ds(pl.multiple_of(core * half, half), half),
            pl.ds(pl.multiple_of(group * width, width), width),
        ],
        exch_tile,
        local_sem.at[0],
    )
    exch_copy.start()
    coulomb_copy = pltpu.make_async_copy(coulomb, coulomb_here, local_sem.at[1])
    coulomb_copy.start()

    trial_full[:, own_columns, :] = trial[...].astype(BF16)

    barrier = pltpu.get_barrier_semaphore()
    for step in range(1, bands):
        pl.semaphore_signal(
            barrier,
            inc=1,
            device_id=(me, lax.rem(band + step, bands)),
            device_id_type=pl.DeviceIdType.MESH,
        )
    for step in range(1, kpoints):
        pl.semaphore_signal(
            barrier,
            inc=1,
            device_id=(lax.rem(me + step, kpoints), band),
            device_id_type=pl.DeviceIdType.MESH,
        )
    pl.semaphore_wait(barrier, bands + kpoints - 2)

    own_rows = pl.ds(pl.multiple_of(band * rows, rows), rows)
    trial_copies = []
    for step in range(1, bands):
        copy = remote(
            trial_full.at[:, own_columns],
            trial_full.at[:, own_columns],
            trial_sem,
            step,
            (me, lax.rem(band + step, bands)),
        )
        copy.start()
        trial_copies.append(copy)
    occ_copies = []
    for step in range(1, bands):
        copy = remote(
            occ, occ_full.at[own_rows], occ_band_sem, step, (me, lax.rem(band + step, bands))
        )
        copy.start()
        occ_copies.append(copy)
    occ_full[own_rows, :] = occ[...]

    for copy in trial_copies:
        copy.wait_recv()
    for v in range(vectors):
        half_own[:, v * occupied : (v + 1) * occupied] = jnp.dot(
            vir[...], trial_full[v], preferred_element_type=F32
        ).astype(BF16)
    half_all[me] = half_own[pl.ds(pl.multiple_of(core * half, half), half), :]
    half_rows = [half_own.at[pl.ds(side * half, half)] for side in range(2)]
    signs = (1, -1)
    half_copies = [
        remote(
            half_own.at[pl.ds(pl.multiple_of((1 - core) * half, half), half)],
            half_all.at[me],
            half_sem,
            0,
            (sibling, band),
        )
    ]
    for way, sign in enumerate(signs):
        next_group = lax.rem(group + sign + groups, groups)
        for side in range(2):
            half_copies.append(
                remote(
                    half_rows[side],
                    half_all.at[me],
                    half_sem,
                    1 + 2 * way + core,
                    (next_group * 2 + side, band),
                    send_slot=1 + 2 * way + side,
                )
            )
    for copy in half_copies[1:] + half_copies[:1]:
        copy.start()

    def half_arrival(distance, way, owner_core):
        source = lax.rem(group - signs[way] * distance + groups, groups) * 2 + owner_core
        slot = (4 * (distance - 1) + 2 * way + owner_core) + 1
        return source, slot

    for copy in occ_copies:
        copy.wait_recv()
    point_copies = []
    for step in range(1, groups):
        peer_group = lax.rem(group + step, groups)
        copy = remote(
            occ_full.at[pl.ds(pl.multiple_of(peer_group * width, width), width)],
            occ_tile.at[me],
            occ_point_sem,
            step,
            (peer_group * 2 + core, band),
        )
        copy.start()
        point_copies.append(copy)
    occ_tile[me] = occ_full[pl.ds(pl.multiple_of(group * width, width), width), :]
    pass_copies = [
        remote(
            occ_full.at[pl.ds(pl.multiple_of(group * width, width), width)],
            occ_tile.at[me],
            occ_pass_sem,
            0,
            (sibling, band),
        )
    ]
    pass_copies[0].start()

    ones = jnp.ones((8, occupied), F32)
    occ_wide = occ[...].astype(F32)
    line = lax.broadcasted_iota(jnp.int32, (8, rows), 0)
    density = jnp.zeros((8, rows), F32)
    for v in range(vectors):
        here = half_own[:, v * occupied : (v + 1) * occupied].astype(F32)
        summed = dot_nt(ones, occ_wide * here, precision=lax.Precision.HIGHEST)
        density = jnp.where(line == v, summed, density)
    dens_all[me] = density
    dens_copies = []
    for step in range(1, kpoints):
        copy = remote(
            dens_all.at[me],
            dens_all.at[me],
            dens_sem,
            step,
            (lax.rem(me + step, kpoints), band),
        )
        copy.start()
        dens_copies.append(copy)

    for step in range(1, groups):
        point_copies[step - 1].wait_recv()
        source = lax.rem(group - step + groups, groups) * 2 + core
        copy = remote(
            occ_tile.at[source], occ_tile.at[source], occ_pass_sem, step, (sibling, band)
        )
        copy.start()
        pass_copies.append(copy)

    def make_pairs(source):
        for v in range(vectors):
            pairs[source * vectors + v] = dot_nt(
                half_all[source, :, v * occupied : (v + 1) * occupied], occ_tile[source]
            )

    arrived = [me, sibling]
    for distance in range(1, groups // 2 + 1):
        for way in range(2):
            for owner_core in range(2):
                if distance == groups // 2 and owner_core != way:
                    continue
                source, slot = half_arrival(distance, way, owner_core)
                here = half_all.at[source]
                remote(here, here, half_sem, slot, (sibling, band)).wait_recv()
                arrived.append(source)
                farther = distance + 1
                if farther < groups // 2 or (farther == groups // 2 and owner_core == way):
                    next_group = lax.rem(group + signs[way] + groups, groups)
                    copy = remote(
                        here, here, half_sem, slot + 4, (next_group * 2 + core, band)
                    )
                    copy.start()
                    half_copies.append(copy)
        if distance == 1:
            vir_turned[...] = vir[...].T
            for copy in dens_copies:
                copy.wait_recv()
            density = dens_all[0]
            for k in range(1, kpoints):
                density += dens_all[k]
            dens_band[band] = jnp.concatenate(
                [density, jnp.zeros_like(density)], axis=0
            ).astype(BF16)
            dens_band_copies = []
            for step in range(1, bands):
                copy = remote(
                    dens_band.at[band],
                    dens_band.at[band],
                    dens_band_sem,
                    step,
                    (me, lax.rem(band + step, bands)),
                )
                copy.start()
                dens_band_copies.append(copy)
            for copy in pass_copies:
                copy.wait_recv()
            exch_copy.wait()
            there = half_all.at[sibling]
            remote(there, there, half_sem, 0, (sibling, band)).wait_recv()
            for source in arrived:
                make_pairs(source)
        else:
            for source in arrived:
                make_pairs(source)
        arrived = []

    def screen(target):
        sources = [table[target, q] * vectors for q in range(kpoints)]

        def add_rows(chunk, carry):
            here = pl.ds(pl.multiple_of(chunk * CHUNK, CHUNK), CHUNK)
            totals = [jnp.zeros((CHUNK, width), F32) for _ in range(vectors)]
            for q in range(kpoints):
                factor = exch_tile[q, here, :].astype(F32)
                for v in range(vectors):
                    totals[v] += pairs[sources[q] + v, here, :] * factor
            for v in range(vectors):
                screened[v, here, :] = totals[v].astype(BF16)
            return carry

        lax.fori_loop(0, half // CHUNK, add_rows, 0)
        return jnp.concatenate(
            [
                jnp.dot(screened[v], occ_tile[target], preferred_element_type=F32)
                for v in range(vectors)
            ],
            axis=1,
        )

    stages = []
    for distance in range(groups // 2, 0, -1):
        level = [
            (distance, way, target_core)
            for way in range(2)
            for target_core in range(2)
            if distance < groups // 2 or target_core == way
        ]
        stages += sorted(level, key=lambda stage: stage[1] == stage[2])
    sums_copies = []
    for slot, (distance, way, target_core) in enumerate(stages):
        sign = signs[way]
        target = lax.rem(group + sign * distance + groups, groups) * 2 + target_core
        total = screen(target)
        earlier = (distance + 1, way, target_core)
        if earlier in stages:
            before = stages.index(earlier)
            there = sums_part.at[before]
            remote(there, there, part_sem, before, (sibling, band)).wait_recv()
            total += sums_part[before].astype(F32)
        sums_send[slot] = total.astype(BF16)
        next_group = lax.rem(group + sign + groups, groups)
        if distance > 1:
            copy = remote(
                sums_send.at[slot],
                sums_part.at[slot],
                part_sem,
                slot,
                (next_group * 2 + core, band),
            )
        else:
            copy = remote(
                sums_send.at[slot],
                sums_recv.at[1 + way, core],
                sums_sem,
                2 + 2 * way + core,
                (next_group * 2 + target_core, band),
                send_slot=2 + 2 * way + target_core,
            )
        copy.start()
        sums_copies.append(copy)
    last = len(stages)
    sums_send[last] = screen(sibling).astype(BF16)
    copy = remote(
        sums_send.at[last],
        sums_recv.at[0, core],
        sums_sem,
        0,
        (sibling, band),
    )
    copy.start()
    sums_copies.append(copy)
    sums_recv[0, core] = screen(me).astype(BF16)

    for copy in dens_band_copies:
        copy.wait_recv()
    coulomb_copy.wait()
    potential = dot_nt(coulomb_here[:, :rows], dens_band[0])
    for part in range(1, bands):
        potential += dot_nt(coulomb_here[:, part * rows : (part + 1) * rows], dens_band[part])
    there = sums_recv.at[0, 1 - core]
    remote(there, there, sums_sem, 0, (sibling, band)).wait_recv()
    for way in range(2):
        for side in range(2):
            there = sums_recv.at[1 + way, side]
            remote(there, there, sums_sem, 2 + 2 * way + side, (sibling, band)).wait_recv()
    coupling = []
    for v in range(vectors):
        pieces = []
        for side in range(2):
            part = slice(v * occupied, (v + 1) * occupied)
            total = sums_recv[0, side, :, part].astype(F32)
            for way in range(2):
                total += sums_recv[1 + way, side, :, part].astype(F32)
            lines = slice(side * half, (side + 1) * half)
            pieces.append(2.0 * potential[lines, v : v + 1] * occ_wide[lines] - total)
        coupling.append(jnp.concatenate(pieces, axis=0).astype(BF16))
    coupling = jnp.concatenate(coupling, axis=1)

    def sigma_of(peer):
        peer_columns = pl.ds(pl.multiple_of(peer * columns, columns), columns)
        return jnp.dot(vir_turned[peer_columns, :], coupling, preferred_element_type=F32)

    sigma_copies = []
    for step in range(1, bands):
        peer = lax.rem(band + step, bands)
        sigma_send[step] = sigma_of(peer).astype(BF16)
        copy = remote(sigma_send.at[step], sigma_recv.at[step], sigma_sem, step, (me, peer))
        copy.start()
        sigma_copies.append(copy)
    result = sigma_of(band)
    for step in range(1, bands):
        sigma_copies[step - 1].wait_recv()
        result += sigma_recv[step].astype(F32)
    for v in range(vectors):
        out[v] = result[:, v * occupied : (v + 1) * occupied]

    for copy in (
        trial_copies
        + occ_copies
        + half_copies
        + point_copies
        + pass_copies
        + dens_copies
        + dens_band_copies
        + sigma_copies
        + sums_copies
    ):
        copy.wait_send()


def coupled_part(kpoints, bands, occ, vir, trial, coulomb, exch, table, vectors):
    rows, occupied = occ.shape
    columns = trial.shape[1]
    merged = vectors * occupied
    auxiliary = coulomb.shape[1]
    half = rows // 2
    width = auxiliary * 2 // kpoints
    vmem = pl.BlockSpec(memory_space=pltpu.VMEM)
    hbm = pl.BlockSpec(memory_space=pl.ANY)
    smem = pl.BlockSpec(memory_space=pltpu.SMEM)
    both = pltpu.SemaphoreType.DMA
    return pl.pallas_call(
        functools.partial(kernel, kpoints, bands, vectors),
        out_shape=jax.ShapeDtypeStruct(trial.shape, F32),
        in_specs=[vmem, vmem, vmem, hbm, hbm, smem],
        out_specs=vmem,
        scratch_shapes=[
            pltpu.VMEM((auxiliary, occupied), BF16),
            pltpu.VMEM((kpoints, width, occupied), BF16),
            pltpu.VMEM((vectors, bands * columns, occupied), BF16),
            pltpu.VMEM((bands * columns, rows), BF16),
            pltpu.VMEM((rows, merged), BF16),
            pltpu.VMEM((kpoints, half, merged), BF16),
            pltpu.VMEM((kpoints, 8, rows), F32),
            pltpu.VMEM((bands, 16, rows), BF16),
            pltpu.VMEM((rows, auxiliary), BF16),
            pltpu.VMEM((kpoints, half, width), BF16),
            pltpu.VMEM((kpoints * vectors, half, width), F32),
            pltpu.VMEM((vectors, half, width), BF16),
            pltpu.VMEM((kpoints, half, merged), BF16),
            pltpu.VMEM((kpoints, half, merged), BF16),
            pltpu.VMEM((3, 2, half, merged), BF16),
            pltpu.VMEM((bands, columns, merged), BF16),
            pltpu.VMEM((bands, columns, merged), BF16),
            both((2,)),
            both((2, bands)),
            both((2, bands)),
            both((2, kpoints)),
            both((2, kpoints)),
            both((2, kpoints * 2)),
            both((2, kpoints)),
            both((2, bands)),
            both((2, kpoints)),
            both((2, kpoints)),
            both((2, bands)),
        ],
        compiler_params=pltpu.CompilerParams(
            collective_id=0, has_side_effects=True, vmem_limit_bytes=60 * 2**20
        ),
        name="coupled",
    )(occ, vir, trial, coulomb, exch, table)


def per_device(
    occ_rows, vir_rows, trial_vectors, occ_energy, vir_energy, coulomb, exch_kernel, minus_table
):
    kpoints = lax.axis_size("ka")
    bands = lax.axis_size("band")
    vectors = trial_vectors.shape[1]
    trial_turned = jnp.swapaxes(trial_vectors[0], 1, 2)
    coupled = coupled_part(
        kpoints,
        bands,
        occ_rows[0],
        vir_rows[0],
        trial_turned,
        coulomb,
        exch_kernel,
        minus_table,
        vectors,
    )
    energy_gaps = vir_energy[0][:, None] - occ_energy[0][None, :]
    return jnp.swapaxes(energy_gaps[None] * trial_turned + coupled, 1, 2)[None]


def solution(mesh):
    in_specs = (
        P("ka", "band", None),
        P("ka", "band", None),
        P("ka", None, None, "band"),
        P("ka", None),
        P("ka", "band"),
        P("band", None),
        P(None, "band", None),
        P(),
    )
    out_specs = P("ka", None, None, "band")
    return jax.shard_map(
        per_device, mesh=mesh, in_specs=in_specs, out_specs=out_specs, check_vma=False
    )
```

```python
import functools

import jax
import jax.numpy as jnp
from jax import lax
from jax.experimental import pallas as pl
from jax.experimental.pallas import tpu as pltpu
from jax.sharding import PartitionSpec as P

F32 = jnp.float32
BF16 = jnp.bfloat16
CHUNK = 16


def dot_nt(left, right, **options):
    return lax.dot_general(
        left, right, (((1,), (1,)), ((), ())), preferred_element_type=F32, **options
    )


def kernel(
    kpoints,
    bands,
    vectors,
    occ,
    vir,
    trial,
    coulomb,
    exch,
    table,
    out,
    occ_full,
    occ_tile,
    trial_full,
    vir_turned,
    half_own,
    half_all,
    dens_all,
    dens_band,
    coulomb_here,
    exch_tile,
    pairs,
    screened,
    sums_send,
    sums_part,
    sums_recv,
    sigma_send,
    sigma_recv,
    local_sem,
    occ_band_sem,
    trial_sem,
    occ_point_sem,
    occ_pass_sem,
    half_sem,
    dens_sem,
    dens_band_sem,
    part_sem,
    sums_sem,
    sigma_sem,
):
    me = lax.axis_index("ka")
    band = lax.axis_index("band")
    groups = kpoints // 2
    group = lax.div(me, 2)
    core = lax.rem(me, 2)
    sibling = me + 1 - 2 * core
    rows, occupied = occ.shape
    auxiliary = occ_full.shape[0]
    half = rows // 2
    width = auxiliary // groups
    columns = trial.shape[1]
    piece = rows // groups
    scattered = piece % 128 == 0

    def tile_of(k):
        return lax.rem(k, 2) * groups + lax.div(k, 2)

    own_columns = pl.ds(pl.multiple_of(band * columns, columns), columns)

    def remote(source, target, sems, slot, device, send_slot=None):
        return pltpu.make_async_remote_copy(
            src_ref=source,
            dst_ref=target,
            send_sem=sems.at[0, slot if send_slot is None else send_slot],
            recv_sem=sems.at[1, slot],
            device_id=device,
            device_id_type=pl.DeviceIdType.MESH,
        )

    blocks = bands if scattered else 1
    block = width // blocks
    exch_copies = []
    for part in range(blocks):
        first = part * rows + group * piece if scattered else group * width
        copy = pltpu.make_async_copy(
            exch.at[
                :,
                pl.ds(pl.multiple_of(core * half, half), half),
                pl.ds(pl.multiple_of(first, 128), block),
            ],
            exch_tile.at[:, :, pl.ds(part * block, block)],
            local_sem.at[1 + part],
        )
        copy.start()
        exch_copies.append(copy)
    coulomb_copy = pltpu.make_async_copy(coulomb, coulomb_here, local_sem.at[0])
    coulomb_copy.start()

    trial_full[:, own_columns, :] = trial[...].astype(BF16)

    barrier = pltpu.get_barrier_semaphore()
    for step in range(1, bands):
        pl.semaphore_signal(
            barrier,
            inc=1,
            device_id=(me, lax.rem(band + step, bands)),
            device_id_type=pl.DeviceIdType.MESH,
        )
    for step in range(1, kpoints):
        pl.semaphore_signal(
            barrier,
            inc=1,
            device_id=(lax.rem(me + step, kpoints), band),
            device_id_type=pl.DeviceIdType.MESH,
        )
    pl.semaphore_wait(barrier, bands + kpoints - 2)

    own_rows = pl.ds(pl.multiple_of(band * rows, rows), rows)
    trial_copies = []
    for step in range(1, bands):
        copy = remote(
            trial_full.at[:, own_columns],
            trial_full.at[:, own_columns],
            trial_sem,
            step,
            (me, lax.rem(band + step, bands)),
        )
        copy.start()
        trial_copies.append(copy)
    occ_copies = []
    point_copies = []
    own_piece = pl.ds(pl.multiple_of(band * piece, piece), piece)
    mine = tile_of(me)
    if scattered:
        for step in range(1, groups):
            peer_group = lax.rem(group + step, groups)
            copy = remote(
                occ.at[pl.ds(pl.multiple_of(peer_group * piece, piece), piece)],
                occ_tile.at[mine, own_piece],
                occ_point_sem,
                step,
                (peer_group * 2 + core, band),
            )
            copy.start()
            point_copies.append(copy)
        occ_tile[mine, own_piece, :] = occ[
            pl.ds(pl.multiple_of(group * piece, piece), piece), :
        ]
        for copy in point_copies:
            copy.wait_recv()
        own_tiles = pl.ds(core * groups, groups)
        for step in range(1, bands):
            copy = remote(
                occ_tile.at[own_tiles, own_piece],
                occ_tile.at[own_tiles, own_piece],
                occ_band_sem,
                step,
                (me, lax.rem(band + step, bands)),
            )
            copy.start()
            occ_copies.append(copy)
    else:
        for step in range(1, bands):
            copy = remote(
                occ, occ_full.at[own_rows], occ_band_sem, step, (me, lax.rem(band + step, bands))
            )
            copy.start()
            occ_copies.append(copy)
        occ_full[own_rows, :] = occ[...]

    for copy in trial_copies:
        copy.wait_recv()
    for v in range(vectors):
        half_own[:, v * occupied : (v + 1) * occupied] = jnp.dot(
            vir[...], trial_full[v], preferred_element_type=F32
        ).astype(BF16)
    half_all[me] = half_own[pl.ds(pl.multiple_of(core * half, half), half), :]
    half_rows = [half_own.at[pl.ds(side * half, half)] for side in range(2)]
    signs = (1, -1)
    half_copies = [
        remote(
            half_own.at[pl.ds(pl.multiple_of((1 - core) * half, half), half)],
            half_all.at[me],
            half_sem,
            0,
            (sibling, band),
        )
    ]
    for way, sign in enumerate(signs):
        next_group = lax.rem(group + sign + groups, groups)
        for side in range(2):
            half_copies.append(
                remote(
                    half_rows[side],
                    half_all.at[me],
                    half_sem,
                    1 + 2 * way + core,
                    (next_group * 2 + side, band),
                    send_slot=1 + 2 * way + side,
                )
            )
    for copy in half_copies[1:] + half_copies[:1]:
        copy.start()

    def half_arrival(distance, way, owner_core):
        source = lax.rem(group - signs[way] * distance + groups, groups) * 2 + owner_core
        slot = (4 * (distance - 1) + 2 * way + owner_core) + 1
        return source, slot

    ones = jnp.ones((8, occupied), F32)
    occ_wide = occ[...].astype(F32)
    line = lax.broadcasted_iota(jnp.int32, (8, rows), 0)
    density = jnp.zeros((8, rows), F32)
    for v in range(vectors):
        here = half_own[:, v * occupied : (v + 1) * occupied].astype(F32)
        summed = dot_nt(ones, occ_wide * here, precision=lax.Precision.HIGHEST)
        density = jnp.where(line == v, summed, density)
    dens_all[me] = density
    dens_copies = []
    for step in range(1, kpoints):
        copy = remote(
            dens_all.at[me],
            dens_all.at[me],
            dens_sem,
            step,
            (lax.rem(me + step, kpoints), band),
        )
        copy.start()
        dens_copies.append(copy)

    for copy in occ_copies:
        copy.wait_recv()
    if scattered:
        pass_copies = [
            remote(
                occ_tile.at[own_tiles],
                occ_tile.at[own_tiles],
                occ_pass_sem,
                0,
                (sibling, band),
            )
        ]
        pass_copies[0].start()
    else:
        for step in range(1, groups):
            peer_group = lax.rem(group + step, groups)
            copy = remote(
                occ_full.at[pl.ds(pl.multiple_of(peer_group * width, width), width)],
                occ_tile.at[mine],
                occ_point_sem,
                step,
                (peer_group * 2 + core, band),
            )
            copy.start()
            point_copies.append(copy)
        occ_tile[mine] = occ_full[pl.ds(pl.multiple_of(group * width, width), width), :]
        pass_copies = [
            remote(
                occ_full.at[pl.ds(pl.multiple_of(group * width, width), width)],
                occ_tile.at[mine],
                occ_pass_sem,
                0,
                (sibling, band),
            )
        ]
        pass_copies[0].start()


    for step in range(1, 1 if scattered else groups):
        point_copies[step - 1].wait_recv()
        source = lax.rem(group - step + groups, groups) * 2 + core
        copy = remote(
            occ_tile.at[tile_of(source)], occ_tile.at[tile_of(source)], occ_pass_sem, step, (sibling, band)
        )
        copy.start()
        pass_copies.append(copy)

    def make_pairs(source):
        for v in range(vectors):
            pairs[source * vectors + v] = dot_nt(
                half_all[source, :, v * occupied : (v + 1) * occupied], occ_tile[tile_of(source)]
            )

    arrived = [me, sibling]
    for distance in range(1, groups // 2 + 1):
        for way in range(2):
            for owner_core in range(2):
                if distance == groups // 2 and owner_core != way:
                    continue
                source, slot = half_arrival(distance, way, owner_core)
                here = half_all.at[source]
                remote(here, here, half_sem, slot, (sibling, band)).wait_recv()
                arrived.append(source)
                farther = distance + 1
                if farther < groups // 2 or (farther == groups // 2 and owner_core == way):
                    next_group = lax.rem(group + signs[way] + groups, groups)
                    copy = remote(
                        here, here, half_sem, slot + 4, (next_group * 2 + core, band)
                    )
                    copy.start()
                    half_copies.append(copy)
        if distance == 1:
            vir_turned[...] = vir[...].T
            for copy in dens_copies:
                copy.wait_recv()
            density = dens_all[0]
            for k in range(1, kpoints):
                density += dens_all[k]
            dens_band[band] = jnp.concatenate(
                [density, jnp.zeros_like(density)], axis=0
            ).astype(BF16)
            dens_band_copies = []
            for step in range(1, bands):
                copy = remote(
                    dens_band.at[band],
                    dens_band.at[band],
                    dens_band_sem,
                    step,
                    (me, lax.rem(band + step, bands)),
                )
                copy.start()
                dens_band_copies.append(copy)
            for copy in pass_copies:
                copy.wait_recv()
            for copy in exch_copies:
                copy.wait()
            there = half_all.at[sibling]
            remote(there, there, half_sem, 0, (sibling, band)).wait_recv()
            for source in arrived:
                make_pairs(source)
        else:
            for source in arrived:
                make_pairs(source)
        arrived = []

    def screen(target):
        sources = [table[target, q] * vectors for q in range(kpoints)]

        def add_rows(chunk, carry):
            here = pl.ds(pl.multiple_of(chunk * CHUNK, CHUNK), CHUNK)
            totals = [jnp.zeros((CHUNK, width), F32) for _ in range(vectors)]
            for q in range(kpoints):
                factor = exch_tile[q, here, :].astype(F32)
                for v in range(vectors):
                    totals[v] += pairs[sources[q] + v, here, :] * factor
            for v in range(vectors):
                screened[v, here, :] = totals[v].astype(BF16)
            return carry

        lax.fori_loop(0, half // CHUNK, add_rows, 0)
        return jnp.concatenate(
            [
                jnp.dot(screened[v], occ_tile[tile_of(target)], preferred_element_type=F32)
                for v in range(vectors)
            ],
            axis=1,
        )

    stages = []
    for distance in range(groups // 2, 0, -1):
        level = [
            (distance, way, target_core)
            for way in range(2)
            for target_core in range(2)
            if distance < groups // 2 or target_core == way
        ]
        stages += sorted(level, key=lambda stage: stage[1] == stage[2])
    sums_copies = []
    for slot, (distance, way, target_core) in enumerate(stages):
        sign = signs[way]
        target = lax.rem(group + sign * distance + groups, groups) * 2 + target_core
        total = screen(target)
        earlier = (distance + 1, way, target_core)
        if earlier in stages:
            before = stages.index(earlier)
            there = sums_part.at[before]
            remote(there, there, part_sem, before, (sibling, band)).wait_recv()
            total += sums_part[before].astype(F32)
        sums_send[slot] = total.astype(BF16)
        next_group = lax.rem(group + sign + groups, groups)
        if distance > 1:
            copy = remote(
                sums_send.at[slot],
                sums_part.at[slot],
                part_sem,
                slot,
                (next_group * 2 + core, band),
            )
        else:
            copy = remote(
                sums_send.at[slot],
                sums_recv.at[1 + way, core],
                sums_sem,
                2 + 2 * way + core,
                (next_group * 2 + target_core, band),
                send_slot=2 + 2 * way + target_core,
            )
        copy.start()
        sums_copies.append(copy)
    last = len(stages)
    sums_send[last] = screen(sibling).astype(BF16)
    copy = remote(
        sums_send.at[last],
        sums_recv.at[0, core],
        sums_sem,
        0,
        (sibling, band),
    )
    copy.start()
    sums_copies.append(copy)
    sums_recv[0, core] = screen(me).astype(BF16)

    for copy in dens_band_copies:
        copy.wait_recv()
    coulomb_copy.wait()
    potential = dot_nt(coulomb_here[:, :rows], dens_band[0])
    for part in range(1, bands):
        potential += dot_nt(coulomb_here[:, part * rows : (part + 1) * rows], dens_band[part])
    there = sums_recv.at[0, 1 - core]
    remote(there, there, sums_sem, 0, (sibling, band)).wait_recv()
    for way in range(2):
        for side in range(2):
            there = sums_recv.at[1 + way, side]
            remote(there, there, sums_sem, 2 + 2 * way + side, (sibling, band)).wait_recv()
    coupling = []
    for v in range(vectors):
        pieces = []
        for side in range(2):
            part = slice(v * occupied, (v + 1) * occupied)
            total = sums_recv[0, side, :, part].astype(F32)
            for way in range(2):
                total += sums_recv[1 + way, side, :, part].astype(F32)
            lines = slice(side * half, (side + 1) * half)
            pieces.append(2.0 * potential[lines, v : v + 1] * occ_wide[lines] - total)
        coupling.append(jnp.concatenate(pieces, axis=0).astype(BF16))
    coupling = jnp.concatenate(coupling, axis=1)

    def sigma_of(peer):
        peer_columns = pl.ds(pl.multiple_of(peer * columns, columns), columns)
        return jnp.dot(vir_turned[peer_columns, :], coupling, preferred_element_type=F32)

    sigma_copies = []
    for step in range(1, bands):
        peer = lax.rem(band + step, bands)
        sigma_send[step] = sigma_of(peer).astype(BF16)
        copy = remote(sigma_send.at[step], sigma_recv.at[step], sigma_sem, step, (me, peer))
        copy.start()
        sigma_copies.append(copy)
    result = sigma_of(band)
    for step in range(1, bands):
        sigma_copies[step - 1].wait_recv()
        result += sigma_recv[step].astype(F32)
    for v in range(vectors):
        out[v] = result[:, v * occupied : (v + 1) * occupied]

    for copy in (
        trial_copies
        + occ_copies
        + half_copies
        + point_copies
        + pass_copies
        + dens_copies
        + dens_band_copies
        + sigma_copies
        + sums_copies
    ):
        copy.wait_send()


def coupled_part(kpoints, bands, occ, vir, trial, coulomb, exch, table, vectors):
    rows, occupied = occ.shape
    columns = trial.shape[1]
    merged = vectors * occupied
    auxiliary = coulomb.shape[1]
    half = rows // 2
    width = auxiliary * 2 // kpoints
    vmem = pl.BlockSpec(memory_space=pltpu.VMEM)
    hbm = pl.BlockSpec(memory_space=pl.ANY)
    smem = pl.BlockSpec(memory_space=pltpu.SMEM)
    both = pltpu.SemaphoreType.DMA
    return pl.pallas_call(
        functools.partial(kernel, kpoints, bands, vectors),
        out_shape=jax.ShapeDtypeStruct(trial.shape, F32),
        in_specs=[vmem, vmem, vmem, hbm, hbm, smem],
        out_specs=vmem,
        scratch_shapes=[
            pltpu.VMEM((auxiliary, occupied), BF16),
            pltpu.VMEM((kpoints, width, occupied), BF16),
            pltpu.VMEM((vectors, bands * columns, occupied), BF16),
            pltpu.VMEM((bands * columns, rows), BF16),
            pltpu.VMEM((rows, merged), BF16),
            pltpu.VMEM((kpoints, half, merged), BF16),
            pltpu.VMEM((kpoints, 8, rows), F32),
            pltpu.VMEM((bands, 16, rows), BF16),
            pltpu.VMEM((rows, auxiliary), BF16),
            pltpu.VMEM((kpoints, half, width), BF16),
            pltpu.VMEM((kpoints * vectors, half, width), F32),
            pltpu.VMEM((vectors, half, width), BF16),
            pltpu.VMEM((kpoints, half, merged), BF16),
            pltpu.VMEM((kpoints, half, merged), BF16),
            pltpu.VMEM((3, 2, half, merged), BF16),
            pltpu.VMEM((bands, columns, merged), BF16),
            pltpu.VMEM((bands, columns, merged), BF16),
            both((1 + bands,)),
            both((2, bands)),
            both((2, bands)),
            both((2, kpoints)),
            both((2, kpoints)),
            both((2, kpoints * 2)),
            both((2, kpoints)),
            both((2, bands)),
            both((2, kpoints)),
            both((2, kpoints)),
            both((2, bands)),
        ],
        compiler_params=pltpu.CompilerParams(
            collective_id=0, has_side_effects=True, vmem_limit_bytes=60 * 2**20
        ),
        name="coupled",
    )(occ, vir, trial, coulomb, exch, table)


def per_device(
    occ_rows, vir_rows, trial_vectors, occ_energy, vir_energy, coulomb, exch_kernel, minus_table
):
    kpoints = lax.axis_size("ka")
    bands = lax.axis_size("band")
    vectors = trial_vectors.shape[1]
    trial_turned = jnp.swapaxes(trial_vectors[0], 1, 2)
    coupled = coupled_part(
        kpoints,
        bands,
        occ_rows[0],
        vir_rows[0],
        trial_turned,
        coulomb,
        exch_kernel,
        minus_table,
        vectors,
    )
    energy_gaps = vir_energy[0][:, None] - occ_energy[0][None, :]
    return jnp.swapaxes(energy_gaps[None] * trial_turned + coupled, 1, 2)[None]


def solution(mesh):
    in_specs = (
        P("ka", "band", None),
        P("ka", "band", None),
        P("ka", None, None, "band"),
        P("ka", None),
        P("ka", "band"),
        P("band", None),
        P(None, "band", None),
        P(),
    )
    out_specs = P("ka", None, None, "band")
    return jax.shard_map(
        per_device, mesh=mesh, in_specs=in_specs, out_specs=out_specs, check_vma=False
    )
```
